32 devices in a mesh: parts: 2 (over y), space: 4 (over z), tm: 2 (over x), spin: 2 (over core).
Axes of the slice: x: 2, y: 2, z: 4, core: 2. Of those that a mesh axis runs over, the one named last changes fastest.
Arguments:
- backward: bfloat16 [4, 2, 4, 64, 3, 4, 128], P('parts', 'tm', None, 'spin', None, 'space'), parts along dimension 0, may hold values from -6 to 6
- forward: bfloat16 [4, 2, 4, 64, 3, 4, 128], P('parts', 'tm', None, 'spin', None, 'space'), parts along dimension 0, may hold values from -6 to 6
- gauge_links: bfloat16 [4, 3, 3, 3, 2, 4, 128], P('parts', None, None, None, 'tm', 'space'), parts along dimension 0, may hold values from -2.5 to 2.5
- momenta: int32 [3, 3], replicated, may hold values from -2 to 2
- gamma_list: int32 [16], replicated, may hold values from 0 to 15
Outputs:
- insertion: float32 [4, 3, 16, 2, 64, 64], P('parts', None, None, 'tm', 'space', 'spin'), parts along dimension 0
The draws below stay inside these ranges and needn't reach their ends.
There are 2 independent parts, one for each index of `parts`. The reference program is written for one: setup_inputs(seed, part) draws one part's arguments, and reference() takes and returns one part's arrays. A program takes and returns all parts, laid end to end along the dimension named above; an argument that names none is the same for every part. Nothing has to cross between parts.
All inputs are finite; a program needn't handle non-finite values.
Results may differ from the reference program's by a relative error of at most 0.0056.
Values may be sent and summed in bfloat16 or wider, within the bound.
A program may use at most 64 MiB of HBM per device.

```python
import math
import jax
import jax.numpy as jnp
import numpy as np
from jax import lax

LX = 32
LY = 4
NCOL = 64
NGAM = 16
NMOM = 3
LZ = 4
SLAB = 2


def with_ends(values, rng, low, top_value):
    index_at = [jax.random.randint(jax.random.fold_in(rng, axis), (), 0, length) for axis, length in enumerate(values.shape)]
    widest = values.shape.index(max(values.shape))
    neighbour = index_at[:widest] + [(index_at[widest] + 1) % values.shape[widest]] + index_at[widest + 1:]
    return values.at[tuple(index_at)].set(low).at[tuple(neighbour)].set(top_value)


def block_scale(stream_key, extent, cuts, low, high):
    factor_of = 1.0
    for axis_at, parts in cuts:
        draws = jax.random.uniform(jax.random.fold_in(jax.random.fold_in(stream_key, 6), axis_at), (parts,), jnp.float32, low / len(cuts), high / len(cuts))
        factor_of = factor_of * jnp.repeat(jnp.exp(draws), extent[axis_at] // parts).reshape((-1,) + (1,) * (len(extent) - 1 - axis_at))
    return factor_of


def bell_draw(rng, extent, width, reach, split=(), kind=jnp.bfloat16):
    entries = width * jax.random.normal(rng, extent, jnp.float32)
    if split:
        entries = entries * block_scale(rng, extent, split, -0.22, 0.18)
    return jnp.clip(entries, -reach, reach).astype(kind)


def setup_inputs(seed: int = 0, part: int = 0) -> dict:
    splits = jax.random.split(jax.random.key(seed), 6)
    own_keys = jax.random.split(jax.random.fold_in(splits[5], part), 6)
    return {
        "backward": bell_draw(own_keys[0], (2, SLAB, 4, NCOL, 3, LZ, LX * LY), 1.0, 6.0, ((1, 2), (3, 2), (5, 4))),
        "forward": bell_draw(own_keys[1], (2, SLAB, 4, NCOL, 3, LZ, LX * LY), 1.0, 6.0, ((1, 2), (3, 2), (5, 4))),
        "gauge_links": bell_draw(own_keys[2], (2, 3, 3, 3, SLAB, LZ, LX * LY), 0.41, 2.5, ((4, 2), (5, 4))),
        "momenta": with_ends(jax.random.randint(splits[3], (NMOM, 3), -2, 3), jax.random.fold_in(splits[3], 1), -2, 2).astype(jnp.int32),
        "gamma_list": with_ends(jax.random.randint(splits[4], (NGAM,), 0, 16), jax.random.fold_in(splits[4], 1), 0, 15).astype(jnp.int32),
    }


def gamma_tables():
    zeros = np.zeros((4, 4))
    gx_imag = np.array([[0, 0, 0, 1], [0, 0, 1, 0], [0, -1, 0, 0], [-1, 0, 0, 0]]) * 1.0
    gy_real = np.array([[0, 0, 0, -1], [0, 0, 1, 0], [0, 1, 0, 0], [-1, 0, 0, 0]]) * 1.0
    gz_imag = np.array([[0, 0, 1, 0], [0, 0, 0, -1], [-1, 0, 0, 0], [0, 1, 0, 0]]) * 1.0
    gt_real = np.array([[0, 0, 1, 0], [0, 0, 0, 1], [1, 0, 0, 0], [0, 1, 0, 0]]) * 1.0
    singles = [(zeros, gx_imag), (gy_real, zeros), (zeros, gz_imag), (gt_real, zeros)]
    clif_real = []
    clif_imag = []
    for number in range(16):
        mat_real = np.eye(4)
        mat_imag = np.zeros((4, 4))
        for which in range(4):
            if number >> which & 1:
                other_real, other_imag = singles[which]
                new_real = mat_real @ other_real - mat_imag @ other_imag
                new_imag = mat_real @ other_imag + mat_imag @ other_real
                mat_real, mat_imag = (new_real, new_imag)
        clif_real.append(mat_real)
        clif_imag.append(mat_imag)
    return (singles, (np.stack(clif_real), np.stack(clif_imag)))

def chosen_gammas(gamma_list):
    singles, clifford = gamma_tables()
    table_real = jnp.asarray(clifford[0], dtype=jnp.float32)
    table_imag = jnp.asarray(clifford[1], dtype=jnp.float32)
    one_hot = (gamma_list[:, None] == jnp.arange(16, dtype=jnp.int32)[None, :]).astype(jnp.float32)
    gam_real = jnp.einsum('kg,gsv->ksv', one_hot, table_real, precision=lax.Precision.HIGHEST)
    gam_imag = jnp.einsum('kg,gsv->ksv', one_hot, table_imag, precision=lax.Precision.HIGHEST)
    return (gam_real, gam_imag)

def color_apply(link_real, link_imag, spin_real, spin_imag, dagger):
    outs_real = []
    outs_imag = []
    for c in range(3):
        summed_real = 0.0
        summed_imag = 0.0
        for d in range(3):
            if dagger:
                coef_real = link_real[d, c]
                coef_imag = -link_imag[d, c]
            else:
                coef_real = link_real[c, d]
                coef_imag = link_imag[c, d]
            coef_real = coef_real[..., None, None, :, :]
            coef_imag = coef_imag[..., None, None, :, :]
            part_real = spin_real[..., d, :, :]
            part_imag = spin_imag[..., d, :, :]
            summed_real = summed_real + coef_real * part_real - coef_imag * part_imag
            summed_imag = summed_imag + coef_real * part_imag + coef_imag * part_real
        outs_real.append(summed_real)
        outs_imag.append(summed_imag)
    return (jnp.stack(outs_real, axis=-3), jnp.stack(outs_imag, axis=-3))

def spin_apply(matrix, spin_real, spin_imag):
    outs_real = []
    outs_imag = []
    for t in range(4):
        summed_real = 0.0
        summed_imag = 0.0
        for s in range(4):
            coef_real = float(matrix[0][t, s])
            coef_imag = float(matrix[1][t, s])
            if coef_real == 0.0 and coef_imag == 0.0:
                continue
            part_real = spin_real[..., s, :, :, :, :]
            part_imag = spin_imag[..., s, :, :, :, :]
            summed_real = summed_real + coef_real * part_real - coef_imag * part_imag
            summed_imag = summed_imag + coef_real * part_imag + coef_imag * part_real
        outs_real.append(summed_real)
        outs_imag.append(summed_imag)
    return (jnp.stack(outs_real, axis=-5), jnp.stack(outs_imag, axis=-5))

def plane_roll(spinor, offset, along_y, width_x):
    initial = spinor.shape
    gridded = spinor.reshape(initial[:-1] + (initial[-1] // width_x, width_x))
    gridded = jnp.roll(gridded, offset, axis=-2 if along_y else -1)
    return gridded.reshape(initial)

def current(fwd_real, fwd_imag, link_real, link_imag, up_z, down_z, width_x):
    singles, clifford = gamma_tables()
    summed_real = 0.0
    summed_imag = 0.0
    for direction in range(3):
        single_real, single_imag = singles[direction]
        minus_proj = ((np.eye(4) - single_real) / 2.0, -single_imag / 2.0)
        plus_proj = ((np.eye(4) + single_real) / 2.0, single_imag / 2.0)
        if direction < 2:
            along_y = direction == 1
            up_real = plane_roll(fwd_real, -1, along_y, width_x)
            up_imag = plane_roll(fwd_imag, -1, along_y, width_x)
            back_real, back_imag = color_apply(link_real[direction], link_imag[direction], fwd_real, fwd_imag, True)
            down_real = plane_roll(back_real, 1, along_y, width_x)
            down_imag = plane_roll(back_imag, 1, along_y, width_x)
        else:
            up_real, up_imag = up_z
            down_real, down_imag = down_z
        hop_real, hop_imag = color_apply(link_real[direction], link_imag[direction], up_real, up_imag, False)
        ahead_real, ahead_imag = spin_apply(minus_proj, hop_real, hop_imag)
        behind_real, behind_imag = spin_apply(plus_proj, down_real, down_imag)
        summed_real = summed_real + ahead_real - behind_real
        summed_imag = summed_imag + ahead_imag - behind_imag
    return (summed_real, summed_imag)

def phase_list(momenta, z_start, layers, plane_size, width_x, width_y, full_z):
    sites = jnp.arange(plane_size, dtype=jnp.int32)
    coord_x = sites % width_x
    coord_y = sites // width_x
    coord_z = z_start + jnp.arange(layers, dtype=jnp.int32)
    result = []
    for number in range(momenta.shape[0]):
        frac_plane = jnp.mod(momenta[number, 0] * coord_x, width_x).astype(jnp.float32) / float(width_x)
        frac_plane = frac_plane + jnp.mod(momenta[number, 1] * coord_y, width_y).astype(jnp.float32) / float(width_y)
        frac_depth = jnp.mod(momenta[number, 2] * coord_z, full_z).astype(jnp.float32) / float(full_z)
        result.append(2.0 * math.pi * (frac_depth[:, None] + frac_plane[None, :]))
    return result

def contract(back_piece, weave_re, weave_im, thetas, gam_real, gam_imag, scaling):
    back_real = back_piece[0].astype(jnp.float32)
    back_imag = back_piece[1].astype(jnp.float32)
    slab_times, spins, columns = (back_real.shape[0], back_real.shape[1], back_real.shape[2])
    blocks = []
    for theta in thetas:
        cosine = jnp.cos(theta)
        sine_part = jnp.sin(theta)
        rot_real = lax.optimization_barrier((cosine * back_real - sine_part * back_imag).astype(jnp.bfloat16)).astype(jnp.float32)
        rot_imag = lax.optimization_barrier((sine_part * back_real + cosine * back_imag).astype(jnp.bfloat16)).astype(jnp.float32)
        stacked = jnp.concatenate([rot_real.reshape(slab_times, spins, columns, -1), rot_imag.reshape(slab_times, spins, columns, -1)], axis=-1)
        pair_real = jnp.einsum('usak,uvbk->usvab', stacked, weave_re)
        pair_imag = jnp.einsum('usak,uvbk->usvab', stacked, weave_im)
        out_real = jnp.einsum('ksv,usvab->kuab', gam_real, pair_real, precision=lax.Precision.HIGHEST) - jnp.einsum('ksv,usvab->kuab', gam_imag, pair_imag, precision=lax.Precision.HIGHEST)
        out_imag = jnp.einsum('ksv,usvab->kuab', gam_real, pair_imag, precision=lax.Precision.HIGHEST) + jnp.einsum('ksv,usvab->kuab', gam_imag, pair_real, precision=lax.Precision.HIGHEST)
        blocks.append(jnp.stack([out_real, out_imag]) * scaling)
    return jnp.stack(blocks, axis=1)

def reference(backward, forward, gauge_links, momenta, gamma_list):
    layers = forward.shape[5]
    plane_size = forward.shape[6]
    width_x = LX
    thetas = phase_list(momenta, jnp.int32(0), layers, plane_size, width_x, plane_size // width_x, layers)
    gam_real, gam_imag = chosen_gammas(gamma_list)
    scaling = 1.0 / math.sqrt(3.0 * plane_size * layers)

    def one_time(slices):
        back_slice, fwd_slice, link_slice = slices
        fwd_real = fwd_slice[0][None].astype(jnp.float32)
        fwd_imag = fwd_slice[1][None].astype(jnp.float32)
        link_real = link_slice[0][:, :, :, None].astype(jnp.float32)
        link_imag = link_slice[1][:, :, :, None].astype(jnp.float32)
        up_z = (jnp.roll(fwd_real, -1, axis=-2), jnp.roll(fwd_imag, -1, axis=-2))
        back_real, back_imag = color_apply(link_real[2], link_imag[2], fwd_real, fwd_imag, True)
        down_z = (jnp.roll(back_real, 1, axis=-2), jnp.roll(back_imag, 1, axis=-2))
        weave_real, weave_imag = current(fwd_real, fwd_imag, link_real, link_imag, up_z, down_z, width_x)
        woven_real = lax.optimization_barrier(weave_real.astype(jnp.bfloat16)).astype(jnp.float32)
        woven_imag = lax.optimization_barrier(weave_imag.astype(jnp.bfloat16)).astype(jnp.float32)
        flat_real = woven_real.reshape(woven_real.shape[0], 4, woven_real.shape[2], -1)
        flat_imag = woven_imag.reshape(woven_imag.shape[0], 4, woven_imag.shape[2], -1)
        weave_re = jnp.concatenate([flat_real, flat_imag], axis=-1)
        weave_im = jnp.concatenate([flat_imag, -flat_real], axis=-1)
        result = contract(back_slice[:, None], weave_re, weave_im, thetas, gam_real, gam_imag, scaling)
        return result[:, :, :, 0]
    stacked = lax.map(one_time, (jnp.moveaxis(backward, 1, 0), jnp.moveaxis(forward, 1, 0), jnp.moveaxis(gauge_links, 4, 0)))
    return jnp.moveaxis(stacked, 0, 3)
```

```python
import functools
import math

import jax
import jax.numpy as jnp
import numpy as np
from jax import lax
from jax.experimental import pallas as pl
from jax.experimental.pallas import tpu as pltpu
from jax.sharding import PartitionSpec as P

LX = 32
GROUP = 16


def gamma_tables():
    zeros = np.zeros((4, 4))
    gx_imag = np.array([[0, 0, 0, 1], [0, 0, 1, 0], [0, -1, 0, 0], [-1, 0, 0, 0]]) * 1.0
    gy_real = np.array([[0, 0, 0, -1], [0, 0, 1, 0], [0, 1, 0, 0], [-1, 0, 0, 0]]) * 1.0
    gz_imag = np.array([[0, 0, 1, 0], [0, 0, 0, -1], [-1, 0, 0, 0], [0, 1, 0, 0]]) * 1.0
    gt_real = np.array([[0, 0, 1, 0], [0, 0, 0, 1], [1, 0, 0, 0], [0, 1, 0, 0]]) * 1.0
    singles = [zeros + 1j * gx_imag, gy_real + 0j, 1j * gz_imag, gt_real + 0j]
    basis = []
    for number in range(16):
        matrix = np.eye(4) + 0j
        for which in range(4):
            if number >> which & 1:
                matrix = matrix @ singles[which]
        basis.append(matrix)
    return singles, np.stack(basis)


def unit_times(unit, value):
    real, imag = value
    if unit == 1:
        return real, imag
    if unit == -1:
        return -real, -imag
    if unit == 1j:
        return -imag, real
    return imag, -real


def small_times(matrix, half):
    outs = []
    for row in range(2):
        column = int(np.flatnonzero(matrix[row])[0])
        outs.append([unit_times(complex(matrix[row, column]), value) for value in half[column]])
    return outs


def added(first, second):
    return [
        [(a[0] + b[0], a[1] + b[1]) for a, b in zip(left, right)]
        for left, right in zip(first, second)
    ]


def subtracted(first, second):
    return [
        [(a[0] - b[0], a[1] - b[1]) for a, b in zip(left, right)]
        for left, right in zip(first, second)
    ]


def kernel(
    spaces,
    width_x,
    full_z,
    scaling,
    back_ref,
    fwd_ref,
    link_ref,
    momenta_ref,
    gamma_ref,
    table_ref,
    out_ref,
    other_back,
    links,
    halo_send,
    halo_recv,
    rows_scr,
    weave,
    weave_mm,
    pair,
    chunk_send,
    chunk_recv,
    back_sems,
    halo_send_sems,
    halo_recv_sems,
    chunk_send_sems,
    chunk_recv_sems,
):
    columns = fwd_ref.shape[3]
    plane = fwd_ref.shape[4]
    moments = momenta_ref.shape[0]
    here = lax.axis_index("space")
    core = lax.axis_index("spin")
    after = lax.rem(here + 1, spaces)
    before = lax.rem(here + spaces - 1, spaces)
    singles, _ = gamma_tables()

    barrier = pltpu.get_barrier_semaphore()
    pl.semaphore_signal(barrier, inc=1, device_id={"spin": 1 - core})
    for step in range(1, spaces):
        pl.semaphore_signal(
            barrier, inc=1, device_id={"space": lax.rem(here + step, spaces)}
        )

    for mu in range(3):
        for c in range(3):
            for d in range(3):
                row = ((mu * 3 + c) * 3 + d) * 2
                links[row : row + 2, :] = link_ref[mu, c, d].astype(jnp.float32)

    def link(mu, c, d):
        row = ((mu * 3 + c) * 3 + d) * 2
        return [
            jnp.broadcast_to(links[row + part : row + part + 1, :], (GROUP, plane))
            for part in range(2)
        ]

    def colour(mu, half, dagger):
        outs = [[None] * 3 for _ in range(2)]
        for c in range(3):
            for d in range(3):
                u_real, u_imag = link(mu, d, c) if dagger else link(mu, c, d)
                for spin in range(2):
                    v_real, v_imag = half[spin][d]
                    if dagger:
                        real = u_real * v_real + u_imag * v_imag
                        imag = u_real * v_imag - u_imag * v_real
                    else:
                        real = u_real * v_real - u_imag * v_imag
                        imag = u_real * v_imag + u_imag * v_real
                    held = outs[spin][c]
                    outs[spin][c] = (
                        (real, imag) if held is None else (held[0] + real, held[1] + imag)
                    )
        return outs

    lanes = lax.broadcasted_iota(jnp.int32, (GROUP, plane), 1)
    column_x = lax.rem(lanes, width_x)

    def rolled(value, steps, along_y):
        if along_y:
            return pltpu.roll(value, (steps * width_x) % plane, 1)
        plain = pltpu.roll(value, steps % plane, 1)
        wrapped = pltpu.roll(value, (steps - steps * width_x) % plane, 1)
        edge = 0 if steps == 1 else width_x - 1
        return jnp.where(column_x == edge, wrapped, plain)

    def rolled_half(half, steps, along_y):
        return [
            [tuple(rolled(part, steps, along_y) for part in value) for value in spin]
            for spin in half
        ]

    def spinor(cols):
        return [
            [
                tuple(fwd_ref[part, s, c, cols, :].astype(jnp.float32) for part in range(2))
                for c in range(3)
            ]
            for s in range(4)
        ]

    def group(index):
        return pl.ds(pl.multiple_of(index * GROUP, GROUP), GROUP)

    def halo_group(index, carry):
        cols = group(index)
        psi = spinor(cols)
        turned = small_times(singles[2][:2, 2:], psi[2:])
        minus = subtracted(psi[:2], turned)
        plus = colour(2, added(psi[:2], turned), True)
        for side, half in enumerate((minus, plus)):
            for spin in range(2):
                for c in range(3):
                    for part in range(2):
                        halo_send[side, part, spin, c, cols, :] = half[spin][c][part].astype(
                            jnp.bfloat16
                        )
        return carry

    lax.fori_loop(0, columns // GROUP, halo_group, 0)

    pl.semaphore_wait(barrier, spaces)

    halo_copies = []
    for side, target in ((0, before), (1, after)):
        copy = pltpu.make_async_remote_copy(
            src_ref=halo_send.at[side],
            dst_ref=halo_recv.at[side],
            send_sem=halo_send_sems.at[side],
            recv_sem=halo_recv_sems.at[side],
            device_id={"space": target},
        )
        copy.start()
        halo_copies.append(copy)
    back_copy = pltpu.make_async_remote_copy(
        src_ref=back_ref,
        dst_ref=other_back,
        send_sem=back_sems.at[0],
        recv_sem=back_sems.at[1],
        device_id={"spin": 1 - core},
    )
    back_copy.start()

    def store_weave(cols, full, first):
        for s in range(4):
            for c in range(3):
                for part in range(2):
                    value = full[s][c][part]
                    if not first:
                        value = value + weave[part, s, c, cols, :]
                    weave[part, s, c, cols, :] = value

    def plane_group(index, carry):
        cols = group(index)
        psi = spinor(cols)
        upper = lower = None
        for mu in range(2):
            turned = small_times(singles[mu][:2, 2:], psi[2:])
            ahead = colour(mu, rolled_half(subtracted(psi[:2], turned), -1, mu == 1), False)
            behind = rolled_half(colour(mu, added(psi[:2], turned), True), 1, mu == 1)
            up = subtracted(ahead, behind)
            low = small_times(-singles[mu][2:, :2], added(ahead, behind))
            upper = up if upper is None else added(upper, up)
            lower = low if lower is None else added(lower, low)
        store_weave(cols, upper + lower, True)
        return carry

    lax.fori_loop(0, columns // GROUP, plane_group, 0)

    sites = lax.broadcasted_iota(jnp.int32, (8, plane), 1)
    coord_x = lax.rem(sites, width_x).astype(jnp.float32)
    coord_y = lax.div(sites, width_x).astype(jnp.float32)
    coord_z = here.astype(jnp.float32)
    phases = []
    for number in range(moments):
        momentum = [momenta_ref[number, axis].astype(jnp.float32) for axis in range(3)]
        turns = coord_x * (momentum[0] * (1.0 / width_x))
        turns = turns + coord_y * (momentum[1] * (width_x / plane))
        turns = turns + coord_z * (momentum[2] * (1.0 / full_z))
        theta = (2.0 * math.pi) * (turns - jnp.floor(turns))
        phases.append((jnp.cos(theta)[:1, :], jnp.sin(theta)[:1, :]))

    def arrange(half, source):
        rows = columns * 2 // spaces
        local = columns // rows
        for part in range(2):
            for c in range(3):
                lane = (part * 3 + c) * plane
                for s in range(4):
                    for j in range(local):
                        row = half * 4 * columns + (j * 4 + s) * rows
                        rows_scr[row : row + rows, lane : lane + plane] = source[
                            part, s, c, j * rows : (j + 1) * rows, :
                        ]

    arrange(0, back_ref)

    back_copy.wait_recv()
    arrange(1, other_back)

    for copy in halo_copies:
        copy.wait_recv()

    def depth_group(index, carry):
        cols = group(index)
        received = [
            [
                [
                    tuple(
                        halo_recv[side, part, spin, c, cols, :].astype(jnp.float32)
                        for part in range(2)
                    )
                    for c in range(3)
                ]
                for spin in range(2)
            ]
            for side in range(2)
        ]
        ahead = colour(2, received[0], False)
        behind = received[1]
        upper = subtracted(ahead, behind)
        lower = small_times(-singles[2][2:, :2], added(ahead, behind))
        store_weave(cols, upper + lower, False)
        return carry

    lax.fori_loop(0, columns // GROUP, depth_group, 0)

    local_chunks = spaces // 2
    chunk_rows = 4 * columns // local_chunks
    copies = {}
    for number in range(moments):
        cosine, sine = phases[number]
        for s in range(4):
            for c in range(3):
                real = weave[0, s, c]
                imag = weave[1, s, c]
                turned_real = (cosine * real + sine * imag).astype(jnp.bfloat16)
                turned_imag = (cosine * imag - sine * real).astype(jnp.bfloat16)
                rows_at = slice(s * columns, (s + 1) * columns)
                rows_next = slice((4 + s) * columns, (5 + s) * columns)
                lanes_at = slice(c * plane, (c + 1) * plane)
                lanes_next = slice((3 + c) * plane, (4 + c) * plane)
                weave_mm[number, rows_at, lanes_at] = turned_real
                weave_mm[number, rows_at, lanes_next] = turned_imag
                weave_mm[number, rows_next, lanes_at] = turned_imag
                weave_mm[number, rows_next, lanes_next] = -turned_real
        product = lax.dot_general(
            rows_scr[...],
            weave_mm[number],
            (((1,), (1,)), ((), ())),
            preferred_element_type=jnp.float32,
        )
        for half in range(2):
            owner = core if half == 0 else 1 - core
            for j in range(local_chunks):
                target = owner * local_chunks + j
                top = (half * local_chunks + j) * chunk_rows
                for part in range(2):
                    piece = product[
                        top : top + chunk_rows, part * 4 * columns : (part + 1) * 4 * columns
                    ]
                    pair[number, target, part] = piece
                    chunk_send[number, target, part] = piece.astype(jnp.bfloat16)

        if number > 0:
            send_chunks(number - 1, spaces, here, chunk_send, chunk_recv, chunk_send_sems,
                        chunk_recv_sems, copies)
    tables = [table_ref[gamma_ref[k]] for k in range(gamma_ref.shape[0])]
    send_chunks(moments - 1, spaces, here, chunk_send, chunk_recv, chunk_send_sems,
                chunk_recv_sems, copies)

    rows = chunk_rows // 4
    for number in range(moments):
        total = [pair[number, here, part] for part in range(2)]
        for step in range(1, spaces):
            copies[number, step].wait_recv()
            for part in range(2):
                total[part] = total[part] + chunk_recv[number, step - 1, part].astype(
                    jnp.float32
                )
        total = [value * scaling for value in total]
        spins = [
            [value[s * rows : (s + 1) * rows, :] for s in range(4)] for value in total
        ]
        for k in range(gamma_ref.shape[0]):
            real = imag = None
            for s in range(4):
                g_real = tables[k][s : s + 1, :]
                g_imag = tables[k][4 + s : 5 + s, :]
                one = g_real * spins[0][s] - g_imag * spins[1][s]
                two = g_real * spins[1][s] + g_imag * spins[0][s]
                real = one if real is None else real + one
                imag = two if imag is None else imag + two
            for part, value in enumerate((real, imag)):
                summed = value[:, :columns]
                for other in range(1, 4):
                    summed = summed + value[:, other * columns : (other + 1) * columns]
                out_ref[part, number, k] = summed

    back_copy.wait_send()
    for copy in halo_copies:
        copy.wait_send()
    for copy in copies.values():
        copy.wait_send()


def send_chunks(
    number, spaces, here, chunk_send, chunk_recv, chunk_send_sems, chunk_recv_sems, copies
):
    for step in range(1, spaces):
        target = lax.rem(here + step, spaces)
        copy = pltpu.make_async_remote_copy(
            src_ref=chunk_send.at[number, target],
            dst_ref=chunk_recv.at[number, step - 1],
            send_sem=chunk_send_sems.at[number, step - 1],
            recv_sem=chunk_recv_sems.at[number, step - 1],
            device_id={"space": target},
        )
        copy.start()
        copies[number, step] = copy


def body(mesh, backward, forward, gauge_links, momenta, gamma_list):
    spaces = mesh.shape["space"]
    _, times, _, columns, _, layers, plane = forward.shape
    moments = momenta.shape[0]
    gammas = gamma_list.shape[0]
    rows = columns * mesh.shape["spin"] // spaces
    back = jnp.transpose(backward, (0, 1, 2, 4, 5, 3, 6)).reshape(2, 4, 3, columns, plane)
    fwd = jnp.transpose(forward, (0, 1, 2, 4, 5, 3, 6)).reshape(2, 4, 3, columns, plane)
    link = jnp.transpose(gauge_links, (1, 2, 3, 4, 5, 0, 6)).reshape(3, 3, 3, 2, plane)
    full_z = layers * spaces
    scaling = 0.5 / math.sqrt(3.0 * plane * full_z)
    _, basis = gamma_tables()
    table = np.concatenate([basis.real, basis.imag], axis=1)
    table = np.repeat(table, columns, axis=2).astype(np.float32)
    vmem = pl.BlockSpec(memory_space=pltpu.VMEM)
    smem = pl.BlockSpec(memory_space=pltpu.SMEM)
    out = pl.pallas_call(
        functools.partial(kernel, spaces, LX, full_z, scaling),
        out_shape=jax.ShapeDtypeStruct((2, moments, gammas, rows, columns), jnp.float32),
        in_specs=[vmem, vmem, vmem, smem, smem, vmem],
        out_specs=vmem,
        scratch_shapes=[
            pltpu.VMEM((2, 4, 3, columns, plane), jnp.bfloat16),
            pltpu.VMEM((56, plane), jnp.float32),
            pltpu.VMEM((2, 2, 2, 3, columns, plane), jnp.bfloat16),
            pltpu.VMEM((2, 2, 2, 3, columns, plane), jnp.bfloat16),
            pltpu.VMEM((8 * columns, 6 * plane), jnp.bfloat16),
            pltpu.VMEM((2, 4, 3, columns, plane), jnp.float32),
            pltpu.VMEM((moments, 8 * columns, 6 * plane), jnp.bfloat16),
            pltpu.VMEM((moments, spaces, 2, 4 * rows, 4 * columns), jnp.float32),
            pltpu.VMEM((moments, spaces, 2, 4 * rows, 4 * columns), jnp.bfloat16),
            pltpu.VMEM((moments, spaces - 1, 2, 4 * rows, 4 * columns), jnp.bfloat16),
            pltpu.SemaphoreType.DMA((2,)),
            pltpu.SemaphoreType.DMA((2,)),
            pltpu.SemaphoreType.DMA((2,)),
            pltpu.SemaphoreType.DMA((moments, spaces - 1)),
            pltpu.SemaphoreType.DMA((moments, spaces - 1)),
        ],
        compiler_params=pltpu.CompilerParams(collective_id=0, has_side_effects=True),
    )(back, fwd, link, momenta, gamma_list, table)
    return out.reshape(2, moments, gammas, times, rows, columns)


def solution(mesh):
    in_specs = (
        P("parts", "tm", None, "spin", None, "space", None),
        P("parts", "tm", None, "spin", None, "space", None),
        P("parts", None, None, None, "tm", "space", None),
        P(),
        P(),
    )
    out_specs = P("parts", None, None, "tm", "space", "spin")
    return jax.shard_map(
        functools.partial(body, mesh),
        mesh=mesh,
        in_specs=in_specs,
        out_specs=out_specs,
        check_vma=False,
    )
```

```python
import functools
import math

import jax
import jax.numpy as jnp
import numpy as np
from jax import lax
from jax.experimental import pallas as pl
from jax.experimental.pallas import tpu as pltpu
from jax.sharding import PartitionSpec as P

LX = 32
GROUP = 16


def gamma_tables():
    zeros = np.zeros((4, 4))
    gx_imag = np.array([[0, 0, 0, 1], [0, 0, 1, 0], [0, -1, 0, 0], [-1, 0, 0, 0]]) * 1.0
    gy_real = np.array([[0, 0, 0, -1], [0, 0, 1, 0], [0, 1, 0, 0], [-1, 0, 0, 0]]) * 1.0
    gz_imag = np.array([[0, 0, 1, 0], [0, 0, 0, -1], [-1, 0, 0, 0], [0, 1, 0, 0]]) * 1.0
    gt_real = np.array([[0, 0, 1, 0], [0, 0, 0, 1], [1, 0, 0, 0], [0, 1, 0, 0]]) * 1.0
    singles = [zeros + 1j * gx_imag, gy_real + 0j, 1j * gz_imag, gt_real + 0j]
    basis = []
    for number in range(16):
        matrix = np.eye(4) + 0j
        for which in range(4):
            if number >> which & 1:
                matrix = matrix @ singles[which]
        basis.append(matrix)
    return singles, np.stack(basis)


def unit_times(unit, value):
    real, imag = value
    if unit == 1:
        return real, imag
    if unit == -1:
        return -real, -imag
    if unit == 1j:
        return -imag, real
    return imag, -real


def small_times(matrix, half):
    outs = []
    for row in range(2):
        column = int(np.flatnonzero(matrix[row])[0])
        outs.append([unit_times(complex(matrix[row, column]), value) for value in half[column]])
    return outs


def added(first, second):
    return [
        [(a[0] + b[0], a[1] + b[1]) for a, b in zip(left, right)]
        for left, right in zip(first, second)
    ]


def subtracted(first, second):
    return [
        [(a[0] - b[0], a[1] - b[1]) for a, b in zip(left, right)]
        for left, right in zip(first, second)
    ]


def kernel(
    spaces,
    width_x,
    full_z,
    scaling,
    back_hbm,
    fwd_hbm,
    link_hbm,
    momenta_ref,
    gamma_ref,
    table_ref,
    out_ref,
    chosen_ref,
    back_ref,
    fwd_ref,
    link_ref,
    other_back,
    links,
    halo_send,
    halo_recv,
    rows_scr,
    weave,
    weave_mm,
    pair,
    chunk_send,
    chunk_recv,
    load_sems,
    back_sems,
    halo_send_sems,
    halo_recv_sems,
    chunk_send_sems,
    chunk_recv_sems,
):
    loads = [
        pltpu.make_async_copy(source, target, load_sems.at[number])
        for number, (source, target) in enumerate(
            ((fwd_hbm, fwd_ref), (link_hbm, link_ref), (back_hbm, back_ref))
        )
    ]
    for load in loads:
        load.start()
    columns = fwd_ref.shape[3]
    plane = fwd_ref.shape[4]
    moments = momenta_ref.shape[0]
    here = lax.axis_index("space")
    core = lax.axis_index("spin")
    after = lax.rem(here + 1, spaces)
    before = lax.rem(here + spaces - 1, spaces)
    singles, _ = gamma_tables()

    barrier = pltpu.get_barrier_semaphore()
    pl.semaphore_signal(barrier, inc=1, device_id={"spin": 1 - core})
    for step in range(1, spaces):
        pl.semaphore_signal(
            barrier, inc=1, device_id={"space": lax.rem(here + step, spaces)}
        )

    for load in loads[:2]:
        load.wait()
    for mu in range(3):
        for c in range(3):
            for d in range(3):
                row = ((mu * 3 + c) * 3 + d) * 2
                links[row : row + 2, :] = link_ref[mu, c, d].astype(jnp.float32)

    def link(mu, c, d):
        row = ((mu * 3 + c) * 3 + d) * 2
        return [
            jnp.broadcast_to(links[row + part : row + part + 1, :], (GROUP, plane))
            for part in range(2)
        ]

    def colour(mu, half, dagger):
        outs = [[None] * 3 for _ in range(2)]
        for c in range(3):
            for d in range(3):
                u_real, u_imag = link(mu, d, c) if dagger else link(mu, c, d)
                for spin in range(2):
                    v_real, v_imag = half[spin][d]
                    if dagger:
                        real = u_real * v_real + u_imag * v_imag
                        imag = u_real * v_imag - u_imag * v_real
                    else:
                        real = u_real * v_real - u_imag * v_imag
                        imag = u_real * v_imag + u_imag * v_real
                    held = outs[spin][c]
                    outs[spin][c] = (
                        (real, imag) if held is None else (held[0] + real, held[1] + imag)
                    )
        return outs

    lanes = lax.broadcasted_iota(jnp.int32, (GROUP, plane), 1)
    column_x = lax.rem(lanes, width_x)

    def rolled(value, steps, along_y):
        if along_y:
            return pltpu.roll(value, (steps * width_x) % plane, 1)
        plain = pltpu.roll(value, steps % plane, 1)
        wrapped = pltpu.roll(value, (steps - steps * width_x) % plane, 1)
        edge = 0 if steps == 1 else width_x - 1
        return jnp.where(column_x == edge, wrapped, plain)

    def rolled_half(half, steps, along_y):
        return [
            [tuple(rolled(part, steps, along_y) for part in value) for value in spin]
            for spin in half
        ]

    def spinor(cols):
        return [
            [
                tuple(fwd_ref[part, s, c, cols, :].astype(jnp.float32) for part in range(2))
                for c in range(3)
            ]
            for s in range(4)
        ]

    def group(index):
        return pl.ds(pl.multiple_of(index * GROUP, GROUP), GROUP)

    def halo_group(index, carry):
        cols = group(index)
        psi = spinor(cols)
        turned = small_times(singles[2][:2, 2:], psi[2:])
        minus = subtracted(psi[:2], turned)
        plus = colour(2, added(psi[:2], turned), True)
        for side, half in enumerate((minus, plus)):
            for spin in range(2):
                for c in range(3):
                    for part in range(2):
                        halo_send[side, part, spin, c, cols, :] = half[spin][c][part].astype(
                            jnp.bfloat16
                        )
        return carry

    lax.fori_loop(0, columns // GROUP, halo_group, 0)

    pl.semaphore_wait(barrier, spaces)

    halo_copies = []
    for side, target in ((0, before), (1, after)):
        copy = pltpu.make_async_remote_copy(
            src_ref=halo_send.at[side],
            dst_ref=halo_recv.at[side],
            send_sem=halo_send_sems.at[side],
            recv_sem=halo_recv_sems.at[side],
            device_id={"space": target},
        )
        copy.start()
        halo_copies.append(copy)
    loads[2].wait()
    back_copy = pltpu.make_async_remote_copy(
        src_ref=back_ref,
        dst_ref=other_back,
        send_sem=back_sems.at[0],
        recv_sem=back_sems.at[1],
        device_id={"spin": 1 - core},
    )
    back_copy.start()

    def store_weave(cols, full, first):
        for s in range(4):
            for c in range(3):
                for part in range(2):
                    value = full[s][c][part]
                    if not first:
                        value = value + weave[part, s, c, cols, :]
                    weave[part, s, c, cols, :] = value

    def plane_group(index, carry):
        cols = group(index)
        psi = spinor(cols)
        upper = lower = None
        for mu in range(2):
            turned = small_times(singles[mu][:2, 2:], psi[2:])
            ahead = colour(mu, rolled_half(subtracted(psi[:2], turned), -1, mu == 1), False)
            behind = rolled_half(colour(mu, added(psi[:2], turned), True), 1, mu == 1)
            up = subtracted(ahead, behind)
            low = small_times(-singles[mu][2:, :2], added(ahead, behind))
            upper = up if upper is None else added(upper, up)
            lower = low if lower is None else added(lower, low)
        store_weave(cols, upper + lower, True)
        return carry

    lax.fori_loop(0, columns // GROUP, plane_group, 0)

    sites = lax.broadcasted_iota(jnp.int32, (8, plane), 1)
    coord_x = lax.rem(sites, width_x).astype(jnp.float32)
    coord_y = lax.div(sites, width_x).astype(jnp.float32)
    coord_z = here.astype(jnp.float32)
    phases = []
    for number in range(moments):
        momentum = [momenta_ref[number, axis].astype(jnp.float32) for axis in range(3)]
        turns = coord_x * (momentum[0] * (1.0 / width_x))
        turns = turns + coord_y * (momentum[1] * (width_x / plane))
        turns = turns + coord_z * (momentum[2] * (1.0 / full_z))
        theta = (2.0 * math.pi) * (turns - jnp.floor(turns))
        phases.append((jnp.cos(theta)[:1, :], jnp.sin(theta)[:1, :]))

    def arrange(half, source):
        rows = columns * 2 // spaces
        local = columns // rows
        for part in range(2):
            for c in range(3):
                lane = (part * 3 + c) * plane
                for s in range(4):
                    for j in range(local):
                        row = half * 4 * columns + (j * 4 + s) * rows
                        rows_scr[row : row + rows, lane : lane + plane] = source[
                            part, s, c, j * rows : (j + 1) * rows, :
                        ]

    arrange(0, back_ref)

    back_copy.wait_recv()
    arrange(1, other_back)

    for copy in halo_copies:
        copy.wait_recv()

    def depth_group(index, carry):
        cols = group(index)
        received = [
            [
                [
                    tuple(
                        halo_recv[side, part, spin, c, cols, :].astype(jnp.float32)
                        for part in range(2)
                    )
                    for c in range(3)
                ]
                for spin in range(2)
            ]
            for side in range(2)
        ]
        ahead = colour(2, received[0], False)
        behind = received[1]
        upper = subtracted(ahead, behind)
        lower = small_times(-singles[2][2:, :2], added(ahead, behind))
        store_weave(cols, upper + lower, False)
        return carry

    lax.fori_loop(0, columns // GROUP, depth_group, 0)

    local_chunks = spaces // 2
    chunk_rows = 4 * columns // local_chunks
    copies = {}
    for number in range(moments):
        cosine, sine = phases[number]
        for s in range(4):
            for c in range(3):
                real = weave[0, s, c]
                imag = weave[1, s, c]
                turned_real = (cosine * real + sine * imag).astype(jnp.bfloat16)
                turned_imag = (cosine * imag - sine * real).astype(jnp.bfloat16)
                rows_at = slice(s * columns, (s + 1) * columns)
                rows_next = slice((4 + s) * columns, (5 + s) * columns)
                lanes_at = slice(c * plane, (c + 1) * plane)
                lanes_next = slice((3 + c) * plane, (4 + c) * plane)
                weave_mm[number, rows_at, lanes_at] = turned_real
                weave_mm[number, rows_at, lanes_next] = turned_imag
                weave_mm[number, rows_next, lanes_at] = turned_imag
                weave_mm[number, rows_next, lanes_next] = -turned_real
        product = lax.dot_general(
            rows_scr[...],
            weave_mm[number],
            (((1,), (1,)), ((), ())),
            preferred_element_type=jnp.float32,
        )
        for half in range(2):
            owner = core if half == 0 else 1 - core
            for j in range(local_chunks):
                target = owner * local_chunks + j
                top = (half * local_chunks + j) * chunk_rows
                for part in range(2):
                    piece = product[
                        top : top + chunk_rows, part * 4 * columns : (part + 1) * 4 * columns
                    ]
                    pair[number, target, part] = piece
                    chunk_send[number, target, part] = piece.astype(jnp.bfloat16)

        if number > 0:
            send_chunks(number - 1, spaces, here, chunk_send, chunk_recv, chunk_send_sems,
                        chunk_recv_sems, copies)
    for k in range(gamma_ref.shape[0]):
        chosen_ref[k] = table_ref[gamma_ref[k]]
    send_chunks(moments - 1, spaces, here, chunk_send, chunk_recv, chunk_send_sems,
                chunk_recv_sems, copies)

    for number in range(moments):
        total = [pair[number, here, part] for part in range(2)]
        for step in range(1, spaces):
            copies[number, step].wait_recv()
            for part in range(2):
                total[part] = total[part] + chunk_recv[number, step - 1, part].astype(
                    jnp.float32
                )
        for part in range(2):
            out_ref[number, part] = total[part] * scaling

    back_copy.wait_send()
    for copy in halo_copies:
        copy.wait_send()
    for copy in copies.values():
        copy.wait_send()


def insert_kernel(chosen_ref, pair_ref, out_hbm, out_ref, sems):
    moments, gammas, rows, columns = out_ref.shape[1:]
    stores = []
    for number in range(moments):
        spins = [
            [pair_ref[number, part, s * rows : (s + 1) * rows, :] for s in range(4)]
            for part in range(2)
        ]
        for k in range(gammas):
            real = imag = None
            for s in range(4):
                g_real = chosen_ref[k, s : s + 1, :]
                g_imag = chosen_ref[k, 4 + s : 5 + s, :]
                one = g_real * spins[0][s] - g_imag * spins[1][s]
                two = g_real * spins[1][s] + g_imag * spins[0][s]
                real = one if real is None else real + one
                imag = two if imag is None else imag + two
            for part, value in enumerate((real, imag)):
                summed = value[:, :columns]
                for other in range(1, 4):
                    summed = summed + value[:, other * columns : (other + 1) * columns]
                out_ref[part, number, k] = summed
        stores.append(
            pltpu.make_async_copy(out_ref.at[:, number], out_hbm.at[:, number], sems.at[number])
        )
        if number > 0:
            stores[number - 1].start()
    stores[-1].start()
    for store in stores:
        store.wait()


def send_chunks(
    number, spaces, here, chunk_send, chunk_recv, chunk_send_sems, chunk_recv_sems, copies
):
    for step in range(1, spaces):
        target = lax.rem(here + step, spaces)
        copy = pltpu.make_async_remote_copy(
            src_ref=chunk_send.at[number, target],
            dst_ref=chunk_recv.at[number, step - 1],
            send_sem=chunk_send_sems.at[number, step - 1],
            recv_sem=chunk_recv_sems.at[number, step - 1],
            device_id={"space": target},
        )
        copy.start()
        copies[number, step] = copy


def body(mesh, backward, forward, gauge_links, momenta, gamma_list):
    spaces = mesh.shape["space"]
    _, times, _, columns, _, layers, plane = forward.shape
    moments = momenta.shape[0]
    gammas = gamma_list.shape[0]
    rows = columns * mesh.shape["spin"] // spaces
    back = jnp.transpose(backward, (0, 1, 2, 4, 5, 3, 6)).reshape(2, 4, 3, columns, plane)
    fwd = jnp.transpose(forward, (0, 1, 2, 4, 5, 3, 6)).reshape(2, 4, 3, columns, plane)
    link = jnp.transpose(gauge_links, (1, 2, 3, 4, 5, 0, 6)).reshape(3, 3, 3, 2, plane)
    full_z = layers * spaces
    scaling = 0.5 / math.sqrt(3.0 * plane * full_z)
    _, basis = gamma_tables()
    table = np.concatenate([basis.real, basis.imag], axis=1)
    table = np.repeat(table, columns, axis=2).astype(np.float32)
    vmem = pl.BlockSpec(memory_space=pltpu.VMEM)
    anywhere = pl.BlockSpec(memory_space=pl.ANY)
    smem = pl.BlockSpec(memory_space=pltpu.SMEM)
    pairs, chosen = pl.pallas_call(
        functools.partial(kernel, spaces, LX, full_z, scaling),
        out_shape=[
            pltpu.VMEM((moments, 2, 4 * rows, 4 * columns), jnp.float32),
            pltpu.VMEM((gammas,) + table.shape[1:], jnp.float32),
        ],
        in_specs=[anywhere, anywhere, anywhere, smem, smem, vmem],
        out_specs=[vmem, vmem],
        scratch_shapes=[
            pltpu.VMEM(back.shape, back.dtype),
            pltpu.VMEM(fwd.shape, fwd.dtype),
            pltpu.VMEM(link.shape, link.dtype),
            pltpu.VMEM((2, 4, 3, columns, plane), jnp.bfloat16),
            pltpu.VMEM((56, plane), jnp.float32),
            pltpu.VMEM((2, 2, 2, 3, columns, plane), jnp.bfloat16),
            pltpu.VMEM((2, 2, 2, 3, columns, plane), jnp.bfloat16),
            pltpu.VMEM((8 * columns, 6 * plane), jnp.bfloat16),
            pltpu.VMEM((2, 4, 3, columns, plane), jnp.float32),
            pltpu.VMEM((moments, 8 * columns, 6 * plane), jnp.bfloat16),
            pltpu.VMEM((moments, spaces, 2, 4 * rows, 4 * columns), jnp.float32),
            pltpu.VMEM((moments, spaces, 2, 4 * rows, 4 * columns), jnp.bfloat16),
            pltpu.VMEM((moments, spaces - 1, 2, 4 * rows, 4 * columns), jnp.bfloat16),
            pltpu.SemaphoreType.DMA((3,)),
            pltpu.SemaphoreType.DMA((2,)),
            pltpu.SemaphoreType.DMA((2,)),
            pltpu.SemaphoreType.DMA((2,)),
            pltpu.SemaphoreType.DMA((moments, spaces - 1)),
            pltpu.SemaphoreType.DMA((moments, spaces - 1)),
        ],
        compiler_params=pltpu.CompilerParams(collective_id=0, has_side_effects=True),
    )(back, fwd, link, momenta, gamma_list, table)
    out_shape = (2, moments, gammas, rows, columns)
    out = pl.pallas_call(
        insert_kernel,
        out_shape=jax.ShapeDtypeStruct(out_shape, jnp.float32),
        in_specs=[vmem, vmem],
        out_specs=anywhere,
        scratch_shapes=[
            pltpu.VMEM(out_shape, jnp.float32),
            pltpu.SemaphoreType.DMA((moments,)),
        ],
    )(
        pltpu.with_memory_space_constraint(chosen, pltpu.VMEM),
        pltpu.with_memory_space_constraint(pairs, pltpu.VMEM),
    )
    return out.reshape(2, moments, gammas, times, rows, columns)


def solution(mesh):
    in_specs = (
        P("parts", "tm", None, "spin", None, "space", None),
        P("parts", "tm", None, "spin", None, "space", None),
        P("parts", None, None, None, "tm", "space", None),
        P(),
        P(),
    )
    out_specs = P("parts", None, None, "tm", "space", "spin")
    return jax.shard_map(
        functools.partial(body, mesh),
        mesh=mesh,
        in_specs=in_specs,
        out_specs=out_specs,
        check_vma=False,
    )
```

```python
import functools
import math

import jax
import jax.numpy as jnp
import numpy as np
from jax import lax
from jax.experimental import pallas as pl
from jax.experimental.pallas import tpu as pltpu
from jax.sharding import PartitionSpec as P

LX = 32
GROUP = 16


def gamma_tables():
    zeros = np.zeros((4, 4))
    gx_imag = np.array([[0, 0, 0, 1], [0, 0, 1, 0], [0, -1, 0, 0], [-1, 0, 0, 0]]) * 1.0
    gy_real = np.array([[0, 0, 0, -1], [0, 0, 1, 0], [0, 1, 0, 0], [-1, 0, 0, 0]]) * 1.0
    gz_imag = np.array([[0, 0, 1, 0], [0, 0, 0, -1], [-1, 0, 0, 0], [0, 1, 0, 0]]) * 1.0
    gt_real = np.array([[0, 0, 1, 0], [0, 0, 0, 1], [1, 0, 0, 0], [0, 1, 0, 0]]) * 1.0
    singles = [zeros + 1j * gx_imag, gy_real + 0j, 1j * gz_imag, gt_real + 0j]
    basis = []
    for number in range(16):
        matrix = np.eye(4) + 0j
        for which in range(4):
            if number >> which & 1:
                matrix = matrix @ singles[which]
        basis.append(matrix)
    return singles, np.stack(basis)


def unit_times(unit, value):
    real, imag = value
    if unit == 1:
        return real, imag
    if unit == -1:
        return -real, -imag
    if unit == 1j:
        return -imag, real
    return imag, -real


def small_times(matrix, half):
    outs = []
    for row in range(2):
        column = int(np.flatnonzero(matrix[row])[0])
        outs.append([unit_times(complex(matrix[row, column]), value) for value in half[column]])
    return outs


def added(first, second):
    return [
        [(a[0] + b[0], a[1] + b[1]) for a, b in zip(left, right)]
        for left, right in zip(first, second)
    ]


def subtracted(first, second):
    return [
        [(a[0] - b[0], a[1] - b[1]) for a, b in zip(left, right)]
        for left, right in zip(first, second)
    ]


def kernel(
    spaces,
    width_x,
    full_z,
    scaling,
    back_hbm,
    fwd_hbm,
    link_hbm,
    momenta_ref,
    gamma_ref,
    table_ref,
    out_ref,
    chosen_ref,
    back_ref,
    fwd_ref,
    link_ref,
    other_back,
    links,
    halo_send,
    halo_recv,
    rows_scr,
    weave,
    weave_mm,
    pair,
    chunk_send,
    chunk_recv,
    relay_recv,
    load_sems,
    back_sems,
    halo_send_sems,
    halo_recv_sems,
    chunk_send_sems,
    chunk_recv_sems,
    relay_send_sems,
    relay_recv_sems,
):
    relay_sems = (relay_send_sems, relay_recv_sems)
    loads = [
        pltpu.make_async_copy(source, target, load_sems.at[number])
        for number, (source, target) in enumerate(
            ((fwd_hbm, fwd_ref), (link_hbm, link_ref), (back_hbm, back_ref))
        )
    ]
    for load in loads:
        load.start()
    columns = fwd_ref.shape[3]
    plane = fwd_ref.shape[4]
    moments = momenta_ref.shape[0]
    here = lax.axis_index("space")
    core = lax.axis_index("spin")
    after = lax.rem(here + 1, spaces)
    before = lax.rem(here + spaces - 1, spaces)
    singles, _ = gamma_tables()

    barrier = pltpu.get_barrier_semaphore()
    pl.semaphore_signal(barrier, inc=1, device_id={"spin": 1 - core})
    for step in range(1, spaces):
        pl.semaphore_signal(
            barrier, inc=1, device_id={"space": lax.rem(here + step, spaces)}
        )

    for load in loads[:2]:
        load.wait()
    for mu in range(3):
        for c in range(3):
            for d in range(3):
                row = ((mu * 3 + c) * 3 + d) * 2
                links[row : row + 2, :] = link_ref[mu, c, d].astype(jnp.float32)

    def link(mu, c, d):
        row = ((mu * 3 + c) * 3 + d) * 2
        return [
            jnp.broadcast_to(links[row + part : row + part + 1, :], (GROUP, plane))
            for part in range(2)
        ]

    def colour(mu, half, dagger):
        outs = [[None] * 3 for _ in range(2)]
        for c in range(3):
            for d in range(3):
                u_real, u_imag = link(mu, d, c) if dagger else link(mu, c, d)
                for spin in range(2):
                    v_real, v_imag = half[spin][d]
                    if dagger:
                        real = u_real * v_real + u_imag * v_imag
                        imag = u_real * v_imag - u_imag * v_real
                    else:
                        real = u_real * v_real - u_imag * v_imag
                        imag = u_real * v_imag + u_imag * v_real
                    held = outs[spin][c]
                    outs[spin][c] = (
                        (real, imag) if held is None else (held[0] + real, held[1] + imag)
                    )
        return outs

    lanes = lax.broadcasted_iota(jnp.int32, (GROUP, plane), 1)
    column_x = lax.rem(lanes, width_x)

    def rolled(value, steps, along_y):
        if along_y:
            return pltpu.roll(value, (steps * width_x) % plane, 1)
        plain = pltpu.roll(value, steps % plane, 1)
        wrapped = pltpu.roll(value, (steps - steps * width_x) % plane, 1)
        edge = 0 if steps == 1 else width_x - 1
        return jnp.where(column_x == edge, wrapped, plain)

    def rolled_half(half, steps, along_y):
        return [
            [tuple(rolled(part, steps, along_y) for part in value) for value in spin]
            for spin in half
        ]

    def spinor(cols):
        return [
            [
                tuple(fwd_ref[part, s, c, cols, :].astype(jnp.float32) for part in range(2))
                for c in range(3)
            ]
            for s in range(4)
        ]

    def group(index):
        return pl.ds(pl.multiple_of(index * GROUP, GROUP), GROUP)

    def halo_group(index, carry):
        cols = group(index)
        psi = spinor(cols)
        turned = small_times(singles[2][:2, 2:], psi[2:])
        minus = subtracted(psi[:2], turned)
        plus = colour(2, added(psi[:2], turned), True)
        for side, half in enumerate((minus, plus)):
            for spin in range(2):
                for c in range(3):
                    for part in range(2):
                        halo_send[side, part, spin, c, cols, :] = half[spin][c][part].astype(
                            jnp.bfloat16
                        )
        return carry

    lax.fori_loop(0, columns // GROUP, halo_group, 0)

    pl.semaphore_wait(barrier, spaces)

    halo_copies = []
    for side, target in ((0, before), (1, after)):
        copy = pltpu.make_async_remote_copy(
            src_ref=halo_send.at[side],
            dst_ref=halo_recv.at[side],
            send_sem=halo_send_sems.at[side],
            recv_sem=halo_recv_sems.at[side],
            device_id={"space": target},
        )
        copy.start()
        halo_copies.append(copy)
    loads[2].wait()
    back_copy = pltpu.make_async_remote_copy(
        src_ref=back_ref,
        dst_ref=other_back,
        send_sem=back_sems.at[0],
        recv_sem=back_sems.at[1],
        device_id={"spin": 1 - core},
    )
    back_copy.start()

    def store_weave(cols, full, first):
        for s in range(4):
            for c in range(3):
                for part in range(2):
                    value = full[s][c][part]
                    if not first:
                        value = value + weave[part, s, c, cols, :]
                    weave[part, s, c, cols, :] = value

    def plane_group(index, carry):
        cols = group(index)
        psi = spinor(cols)
        upper = lower = None
        for mu in range(2):
            turned = small_times(singles[mu][:2, 2:], psi[2:])
            ahead = colour(mu, rolled_half(subtracted(psi[:2], turned), -1, mu == 1), False)
            behind = rolled_half(colour(mu, added(psi[:2], turned), True), 1, mu == 1)
            up = subtracted(ahead, behind)
            low = small_times(-singles[mu][2:, :2], added(ahead, behind))
            upper = up if upper is None else added(upper, up)
            lower = low if lower is None else added(lower, low)
        store_weave(cols, upper + lower, True)
        return carry

    lax.fori_loop(0, columns // GROUP, plane_group, 0)

    sites = lax.broadcasted_iota(jnp.int32, (8, plane), 1)
    coord_x = lax.rem(sites, width_x).astype(jnp.float32)
    coord_y = lax.div(sites, width_x).astype(jnp.float32)
    coord_z = here.astype(jnp.float32)
    phases = []
    for number in range(moments):
        momentum = [momenta_ref[number, axis].astype(jnp.float32) for axis in range(3)]
        turns = coord_x * (momentum[0] * (1.0 / width_x))
        turns = turns + coord_y * (momentum[1] * (width_x / plane))
        turns = turns + coord_z * (momentum[2] * (1.0 / full_z))
        theta = (2.0 * math.pi) * (turns - jnp.floor(turns))
        phases.append((jnp.cos(theta)[:1, :], jnp.sin(theta)[:1, :]))

    def arrange(half, source):
        rows = columns * 2 // spaces
        local = columns // rows
        for part in range(2):
            for c in range(3):
                lane = (part * 3 + c) * plane
                for s in range(4):
                    for j in range(local):
                        row = half * 4 * columns + (j * 4 + s) * rows
                        rows_scr[row : row + rows, lane : lane + plane] = source[
                            part, s, c, j * rows : (j + 1) * rows, :
                        ]

    arrange(0, back_ref)

    back_copy.wait_recv()
    arrange(1, other_back)

    for copy in halo_copies:
        copy.wait_recv()

    def depth_group(index, carry):
        cols = group(index)
        received = [
            [
                [
                    tuple(
                        halo_recv[side, part, spin, c, cols, :].astype(jnp.float32)
                        for part in range(2)
                    )
                    for c in range(3)
                ]
                for spin in range(2)
            ]
            for side in range(2)
        ]
        ahead = colour(2, received[0], False)
        behind = received[1]
        upper = subtracted(ahead, behind)
        lower = small_times(-singles[2][2:, :2], added(ahead, behind))
        store_weave(cols, upper + lower, False)
        return carry

    lax.fori_loop(0, columns // GROUP, depth_group, 0)

    local_chunks = spaces // 2
    chunk_rows = 4 * columns // local_chunks
    copies = {}
    relays = {}
    for number in range(moments):
        cosine, sine = phases[number]
        for s in range(4):
            for c in range(3):
                real = weave[0, s, c]
                imag = weave[1, s, c]
                turned_real = (cosine * real + sine * imag).astype(jnp.bfloat16)
                turned_imag = (cosine * imag - sine * real).astype(jnp.bfloat16)
                rows_at = slice(s * columns, (s + 1) * columns)
                rows_next = slice((4 + s) * columns, (5 + s) * columns)
                lanes_at = slice(c * plane, (c + 1) * plane)
                lanes_next = slice((3 + c) * plane, (4 + c) * plane)
                weave_mm[number, rows_at, lanes_at] = turned_real
                weave_mm[number, rows_at, lanes_next] = turned_imag
                weave_mm[number, rows_next, lanes_at] = turned_imag
                weave_mm[number, rows_next, lanes_next] = -turned_real
        product = lax.dot_general(
            rows_scr[...],
            weave_mm[number],
            (((1,), (1,)), ((), ())),
            preferred_element_type=jnp.float32,
        )
        for half in range(2):
            owner = core if half == 0 else 1 - core
            for j in range(local_chunks):
                target = owner * local_chunks + j
                top = (half * local_chunks + j) * chunk_rows
                for part in range(2):
                    piece = product[
                        top : top + chunk_rows, part * 4 * columns : (part + 1) * 4 * columns
                    ]
                    pair[number, target, part] = piece
                    chunk_send[number, target, part] = piece.astype(jnp.bfloat16)

        if number > 0:
            send_chunks(number - 1, spaces, here, chunk_send, chunk_recv, chunk_send_sems,
                        chunk_recv_sems, copies, relays, relay_recv, relay_sems)
    send_chunks(moments - 1, spaces, here, chunk_send, chunk_recv, chunk_send_sems,
                chunk_recv_sems, copies, relays, relay_recv, relay_sems)

    late = None
    for number in range(moments):
        for part in sorted(relay_steps(spaces)):
            relays[number, part].wait_recv()
            step = relay_steps(spaces)[part]
            target = lax.rem(here + step, spaces)
            joined = pair[number, target, part] + relay_recv[number, part].astype(jnp.float32)
            chunk_send[number, target, part] = joined.astype(jnp.bfloat16)
            if late is not None:
                send_piece(late, spaces, here, chunk_send, chunk_recv, chunk_send_sems,
                           chunk_recv_sems, copies)
            late = (number, step, part)
    for k in range(gamma_ref.shape[0]):
        chosen_ref[k] = table_ref[gamma_ref[k]]
    if late is not None:
        send_piece(late, spaces, here, chunk_send, chunk_recv, chunk_send_sems,
                   chunk_recv_sems, copies)

    for number in range(moments):
        for part in range(2):
            total = pair[number, here, part]
            for step in range(1, spaces):
                if (number, step, part) in copies:
                    copies[number, step, part].wait_recv()
                    total = total + chunk_recv[number, step - 1, part].astype(jnp.float32)
            out_ref[number, part] = total * scaling

    back_copy.wait_send()
    for copy in halo_copies:
        copy.wait_send()
    for copy in (*copies.values(), *relays.values()):
        copy.wait_send()


def insert_kernel(chosen_ref, pair_ref, out_hbm, out_ref, sems):
    moments, gammas, rows, columns = out_ref.shape[1:]
    stores = []
    for number in range(moments):
        spins = [
            [pair_ref[number, part, s * rows : (s + 1) * rows, :] for s in range(4)]
            for part in range(2)
        ]
        for k in range(gammas):
            real = imag = None
            for s in range(4):
                g_real = chosen_ref[k, s : s + 1, :]
                g_imag = chosen_ref[k, 4 + s : 5 + s, :]
                one = g_real * spins[0][s] - g_imag * spins[1][s]
                two = g_real * spins[1][s] + g_imag * spins[0][s]
                real = one if real is None else real + one
                imag = two if imag is None else imag + two
            for part, value in enumerate((real, imag)):
                summed = value[:, :columns]
                for other in range(1, 4):
                    summed = summed + value[:, other * columns : (other + 1) * columns]
                out_ref[part, number, k] = summed
        stores.append(
            pltpu.make_async_copy(out_ref.at[:, number], out_hbm.at[:, number], sems.at[number])
        )
        if number > 0:
            stores[number - 1].start()
    stores[-1].start()
    for store in stores:
        store.wait()


def relay_steps(spaces):
    half = spaces // 2
    return {0: half - 1, 1: spaces - half + 1} if half > 1 else {}


def send_piece(
    piece, spaces, here, chunk_send, chunk_recv, chunk_send_sems, chunk_recv_sems, copies
):
    number, step, part = piece
    target = lax.rem(here + step, spaces)
    copy = pltpu.make_async_remote_copy(
        src_ref=chunk_send.at[number, target, part],
        dst_ref=chunk_recv.at[number, step - 1, part],
        send_sem=chunk_send_sems.at[number, step - 1, part],
        recv_sem=chunk_recv_sems.at[number, step - 1, part],
        device_id={"space": target},
    )
    copy.start()
    copies[piece] = copy


def send_chunks(
    number, spaces, here, chunk_send, chunk_recv, chunk_send_sems, chunk_recv_sems, copies,
    relays, relay_recv, relay_sems,
):
    half = spaces // 2
    merged = relay_steps(spaces)
    for part in merged:
        copy = pltpu.make_async_remote_copy(
            src_ref=chunk_send.at[number, lax.rem(here + half, spaces), part],
            dst_ref=relay_recv.at[number, part],
            send_sem=relay_sems[0].at[number, part],
            recv_sem=relay_sems[1].at[number, part],
            device_id={"space": lax.rem(here + (1 if part == 0 else spaces - 1), spaces)},
        )
        copy.start()
        relays[number, part] = copy
    for step in range(1, spaces):
        for part in range(2):
            if merged and (step == half or merged[part] == step):
                continue
            send_piece((number, step, part), spaces, here, chunk_send, chunk_recv,
                       chunk_send_sems, chunk_recv_sems, copies)


def body(mesh, backward, forward, gauge_links, momenta, gamma_list):
    spaces = mesh.shape["space"]
    _, times, _, columns, _, layers, plane = forward.shape
    moments = momenta.shape[0]
    gammas = gamma_list.shape[0]
    rows = columns * mesh.shape["spin"] // spaces
    back = jnp.transpose(backward, (0, 1, 2, 4, 5, 3, 6)).reshape(2, 4, 3, columns, plane)
    fwd = jnp.transpose(forward, (0, 1, 2, 4, 5, 3, 6)).reshape(2, 4, 3, columns, plane)
    link = jnp.transpose(gauge_links, (1, 2, 3, 4, 5, 0, 6)).reshape(3, 3, 3, 2, plane)
    full_z = layers * spaces
    scaling = 0.5 / math.sqrt(3.0 * plane * full_z)
    _, basis = gamma_tables()
    table = np.concatenate([basis.real, basis.imag], axis=1)
    table = np.repeat(table, columns, axis=2).astype(np.float32)
    vmem = pl.BlockSpec(memory_space=pltpu.VMEM)
    anywhere = pl.BlockSpec(memory_space=pl.ANY)
    smem = pl.BlockSpec(memory_space=pltpu.SMEM)
    pairs, chosen = pl.pallas_call(
        functools.partial(kernel, spaces, LX, full_z, scaling),
        out_shape=[
            pltpu.VMEM((moments, 2, 4 * rows, 4 * columns), jnp.float32),
            pltpu.VMEM((gammas,) + table.shape[1:], jnp.float32),
        ],
        in_specs=[anywhere, anywhere, anywhere, smem, smem, vmem],
        out_specs=[vmem, vmem],
        scratch_shapes=[
            pltpu.VMEM(back.shape, back.dtype),
            pltpu.VMEM(fwd.shape, fwd.dtype),
            pltpu.VMEM(link.shape, link.dtype),
            pltpu.VMEM((2, 4, 3, columns, plane), jnp.bfloat16),
            pltpu.VMEM((56, plane), jnp.float32),
            pltpu.VMEM((2, 2, 2, 3, columns, plane), jnp.bfloat16),
            pltpu.VMEM((2, 2, 2, 3, columns, plane), jnp.bfloat16),
            pltpu.VMEM((8 * columns, 6 * plane), jnp.bfloat16),
            pltpu.VMEM((2, 4, 3, columns, plane), jnp.float32),
            pltpu.VMEM((moments, 8 * columns, 6 * plane), jnp.bfloat16),
            pltpu.VMEM((moments, spaces, 2, 4 * rows, 4 * columns), jnp.float32),
            pltpu.VMEM((moments, spaces, 2, 4 * rows, 4 * columns), jnp.bfloat16),
            pltpu.VMEM((moments, spaces - 1, 2, 4 * rows, 4 * columns), jnp.bfloat16),
            pltpu.VMEM((moments, 2, 4 * rows, 4 * columns), jnp.bfloat16),
            pltpu.SemaphoreType.DMA((3,)),
            pltpu.SemaphoreType.DMA((2,)),
            pltpu.SemaphoreType.DMA((2,)),
            pltpu.SemaphoreType.DMA((2,)),
            pltpu.SemaphoreType.DMA((moments, spaces - 1, 2)),
            pltpu.SemaphoreType.DMA((moments, spaces - 1, 2)),
            pltpu.SemaphoreType.DMA((moments, 2)),
            pltpu.SemaphoreType.DMA((moments, 2)),
        ],
        compiler_params=pltpu.CompilerParams(collective_id=0, has_side_effects=True),
    )(back, fwd, link, momenta, gamma_list, table)
    out_shape = (2, moments, gammas, rows, columns)
    out = pl.pallas_call(
        insert_kernel,
        out_shape=jax.ShapeDtypeStruct(out_shape, jnp.float32),
        in_specs=[vmem, vmem],
        out_specs=anywhere,
        scratch_shapes=[
            pltpu.VMEM(out_shape, jnp.float32),
            pltpu.SemaphoreType.DMA((moments,)),
        ],
    )(
        pltpu.with_memory_space_constraint(chosen, pltpu.VMEM),
        pltpu.with_memory_space_constraint(pairs, pltpu.VMEM),
    )
    return out.reshape(2, moments, gammas, times, rows, columns)


def solution(mesh):
    in_specs = (
        P("parts", "tm", None, "spin", None, "space", None),
        P("parts", "tm", None, "spin", None, "space", None),
        P("parts", None, None, None, "tm", "space", None),
        P(),
        P(),
    )
    out_specs = P("parts", None, None, "tm", "space", "spin")
    return jax.shard_map(
        functools.partial(body, mesh),
        mesh=mesh,
        in_specs=in_specs,
        out_specs=out_specs,
        check_vma=False,
    )
```
